32 devices in a mesh: dom: 8 (over y, x, core), col: 4 (over z).
Axes of the slice: x: 2, y: 2, z: 4, core: 2. Of those that a mesh axis runs over, the one named last changes fastest.
Arguments:
- features: bfloat16 [65536, 1024], P('dom', 'col'), may hold values from -6 to 6
- requests: int32 [8, 8, 8], P('dom'), may hold values from 0 to 63
- counts: int32 [8, 8], P(None, 'dom'), may hold values from 0 to 8, as said below
- tile_block: int32 [128, 32], P('dom'), may hold values from 0 to 31
- local_nbr: int32 [16384, 128], P('dom'), may hold values from 0 to 127
- tile_count: int32 [128], P('dom'), may hold values from 1 to 32, as said below
- w_self: bfloat16 [1024, 1024], P('col'), may hold values from -0.125 to 0.125
- w_neigh: bfloat16 [1024, 1024], P('col'), may hold values from -0.75 to 0.75
Outputs:
- embeddings: bfloat16 [16384, 1024], P('dom', 'col')
The draws below stay inside these ranges and needn't reach their ends.
Inputs may be any that keep to these rules, and one draw needn't show every extreme that they name: Each shard's counts over all partitions sum to 32; for every shard some partition has exactly 8. `tile_count`: on every shard some destination block uses all 32 tiles.
All inputs are finite; a program needn't handle non-finite values.
Results may differ from the reference program's by a relative error of at most 0.014.
Values may be sent and summed in bfloat16 or wider, within the bound.
A program may use at most 128 MiB of HBM per device.

```python
import jax
import jax.numpy as jnp
from jax import lax

D = 1024
BLOCK_ROWS = 128
BLK_DEV = 64
CAP = 8
DST_BLK = 16
TILES = 32
FAN_T = 4
FRONT = 32
BLOCKS = 512
DST_BLOCKS = 128
COL_W = 256
N_DOM = 8


def draw_counts(key, part):
    key_order, key_share, key_heat = jax.random.split(key, 3)
    heat = jax.random.permutation(key_heat, N_DOM)
    orders = jax.vmap(lambda subkey: jax.random.permutation(subkey, N_DOM))(jax.random.split(key_order, N_DOM))
    share = jax.random.randint(key_share, (N_DOM, N_DOM // 2), 0, CAP + 1)
    share = share.at[:, 0].set(CAP)
    first_half = orders[:, 0::2]
    second_half = orders[:, 1::2]
    larger = jnp.maximum(share, CAP - share)
    hotter = heat[first_half] > heat[second_half]
    first_count = jnp.where(hotter, larger, CAP - larger)
    second_count = CAP - first_count
    shard_rows = jnp.arange(N_DOM)[:, None]
    grid = jnp.zeros((N_DOM, N_DOM), jnp.int32)
    grid = grid.at[shard_rows, first_half].set(first_count)
    grid = grid.at[shard_rows, second_half].set(second_count)
    return grid.T.astype(jnp.int32)


def draw_tile_count(key, part):
    key_level, key_raw, key_where = jax.random.split(key, 3)
    levels = jax.random.randint(key_level, (N_DOM, 1), TILES // 4, TILES + 1)
    raw_bits = jax.random.randint(key_raw, (N_DOM, DST_BLK), 0, 1 << 20)
    result = 1 + raw_bits % levels
    full_at = jax.random.randint(key_where, (N_DOM, 1), 0, DST_BLK)
    result = jnp.where(jnp.arange(DST_BLK)[None, :] == full_at, TILES, result)
    return result.reshape(-1).astype(jnp.int32)


def place_ends(drawn, own_key, low, high):
    index_at = [jax.random.randint(jax.random.fold_in(own_key, axis), (), 0, length) for axis, length in enumerate(drawn.shape)]
    main_axis = drawn.shape.index(max(drawn.shape))
    neighbour = index_at[:main_axis] + [(index_at[main_axis] + 1) % drawn.shape[main_axis]] + index_at[main_axis + 1:]
    return drawn.at[tuple(index_at)].set(low).at[tuple(neighbour)].set(high)


def level_of(rng, dims, cuts, low, top_value):
    loudness, own = 1.0, jax.random.fold_in(rng, 6)
    for position, shards_of in cuts:
        heights = jnp.exp(jax.random.uniform(jax.random.fold_in(own, position), (shards_of,), jnp.float32, low / len(cuts), top_value / len(cuts)))
        loudness = loudness * jnp.repeat(heights, dims[position] // shards_of).reshape([-1 if axis == position else 1 for axis in range(len(dims))])
    return loudness


def gaussian(rng, extent, spread, bound, cuts=(), kind=jnp.bfloat16):
    entries = jax.random.normal(rng, extent, jnp.float32) * spread
    if len(cuts) > 0:
        entries = level_of(rng, extent, cuts, -0.22, 0.18) * entries
    return jnp.clip(entries, min=-bound, max=bound).astype(kind)


def setup_inputs(seed: int = 0) -> dict:
    seeds = jax.random.split(jax.random.key(seed), 9)
    return {
        "features": gaussian(seeds[0], (BLOCKS * BLOCK_ROWS, D), 1.0, 6.0, ((0, 8), (1, 4))),
        "requests": place_ends(jax.random.randint(seeds[1], (N_DOM, N_DOM, CAP), 0, BLK_DEV), jax.random.fold_in(seeds[1], 1), 0, BLK_DEV - 1).astype(jnp.int32),
        "counts": draw_counts(jax.random.fold_in(seeds[8], 71), 0),
        "tile_block": place_ends(jax.random.randint(seeds[3], (DST_BLOCKS, TILES), 0, FRONT), jax.random.fold_in(seeds[3], 1), 0, FRONT - 1).astype(jnp.int32),
        "local_nbr": place_ends(jax.random.randint(seeds[4], (DST_BLOCKS * BLOCK_ROWS, TILES * FAN_T), 0, BLOCK_ROWS), jax.random.fold_in(seeds[4], 1), 0, BLOCK_ROWS - 1).astype(jnp.int32),
        "tile_count": draw_tile_count(jax.random.fold_in(seeds[8], 71), 0),
        "w_self": gaussian(seeds[6], (D, D), (2 * D) ** -0.5, 0.125, ((0, 4),)),
        "w_neigh": gaussian(seeds[7], (D, D), (D // 16) ** -0.5, 0.75, ((0, 4),)),
    }


def frontier_blocks(requests, counts):
    slot_ends = jnp.cumsum(counts, axis=0)
    slot_starts = slot_ends - counts
    positions = jnp.arange(FRONT, dtype=jnp.int32)

    def one_shard(ends_col, starts_col, wanted):
        owner_of = lax.optimization_barrier(jnp.sum((ends_col[None, :] <= positions[:, None]).astype(jnp.int32), axis=1))
        slot_pos = positions - starts_col[owner_of]
        return (owner_of * BLK_DEV + wanted[owner_of, slot_pos]).astype(jnp.int32)
    return jax.vmap(one_shard, in_axes=(1, 1, 1))(slot_ends, slot_starts, requests)

def reference(features, requests, counts, tile_block, local_nbr, tile_count, w_self, w_neigh):
    global_block = frontier_blocks(requests, counts)
    tile_ids = jnp.arange(TILES, dtype=jnp.int32)
    row_ids = jnp.arange(BLOCK_ROWS, dtype=jnp.int32)
    groups = D // COL_W
    self_mat = w_self.astype(jnp.float32).reshape(groups, COL_W, D)
    neigh_mat = w_neigh.astype(jnp.float32).reshape(groups, COL_W, D)

    def one_block(inputs):
        block_id, picks, neighbor, used_tiles = inputs
        shard_row = global_block[block_id // DST_BLK]
        tile_global = shard_row[picks]
        rows = tile_global[None, :, None] * BLOCK_ROWS + neighbor.reshape(BLOCK_ROWS, TILES, FAN_T)
        values = features[rows.reshape(-1)].astype(jnp.float32).reshape(BLOCK_ROWS, TILES, FAN_T, D)
        live_mask = (tile_ids < used_tiles).astype(jnp.float32)
        summed = lax.optimization_barrier(jnp.sum(values * live_mask[None, :, None, None], axis=(1, 2)))
        agg = (summed / (FAN_T * used_tiles).astype(jnp.float32)).astype(jnp.bfloat16)
        own = features[shard_row[block_id % DST_BLK] * BLOCK_ROWS + row_ids]
        pieces = jnp.einsum('rkc,kcj->krj', own.astype(jnp.float32).reshape(BLOCK_ROWS, groups, COL_W), self_mat, precision=lax.Precision.HIGHEST)
        pieces = pieces + jnp.einsum('rkc,kcj->krj', agg.astype(jnp.float32).reshape(BLOCK_ROWS, groups, COL_W), neigh_mat, precision=lax.Precision.HIGHEST)
        pieces = lax.optimization_barrier(pieces.astype(jnp.bfloat16)).astype(jnp.float32)
        hidden = jnp.maximum(lax.optimization_barrier(jnp.sum(pieces, axis=0)), 0.0)
        scale = jnp.sqrt(0.25 + lax.optimization_barrier(jnp.sum(hidden * hidden, axis=1, keepdims=True)) / D)
        return (hidden / scale).astype(jnp.bfloat16)
    block_ids = jnp.arange(DST_BLOCKS, dtype=jnp.int32)
    result = lax.map(one_block, (block_ids, tile_block, local_nbr.reshape(DST_BLOCKS, BLOCK_ROWS, TILES * FAN_T), tile_count))
    return result.reshape(DST_BLOCKS * BLOCK_ROWS, D)
```

```python
import functools

import jax
import jax.numpy as jnp
from jax import lax
from jax.experimental import pallas as pl
from jax.experimental.pallas import tpu as pltpu
from jax.sharding import PartitionSpec as P

D = 1024
BLOCK_ROWS = 128
CAP = 8
TILES = 32
FAN_T = 4
GROUP = 4
PACK = 16


def aggregate_kernel(
    front, width, slot_of, tile_block, tile_count, nbr_ref, arrived, out_ref, held, turned, nbr_t, sems
):
    step = pl.program_id(0)

    def fetch(p):
        return pltpu.make_async_copy(arrived.at[slot_of[p]], held.at[p], sems.at[p])

    @pl.when(step == 0)
    def _():
        def begin(p, carry):
            fetch(p).start()
            return carry

        lax.fori_loop(0, front, begin, 0)

        def finish(p, carry):
            fetch(p).wait()
            turned[p] = held[p].T
            return carry

        lax.fori_loop(0, front, finish, 0)

    nbr_t[...] = nbr_ref[...].astype(jnp.float32).T
    used = tile_count[step]
    shape = (BLOCK_ROWS // PACK, PACK, BLOCK_ROWS)
    row_ids = (
        lax.broadcasted_iota(jnp.int32, shape, 0) * PACK + lax.broadcasted_iota(jnp.int32, shape, 1)
    ).astype(jnp.float32).astype(jnp.bfloat16)
    one = jnp.ones(shape, jnp.bfloat16)
    zero = jnp.zeros(shape, jnp.bfloat16)

    def body(q, acc):
        nbr = nbr_t[pl.ds(pl.multiple_of(q * (GROUP * FAN_T), GROUP * FAN_T), GROUP * FAN_T), :]
        counts = []
        blocks = []
        for i in range(GROUP):
            tile = q * GROUP + i
            total = None
            for f in range(FAN_T):
                row = nbr[i * FAN_T + f : i * FAN_T + f + 1, :]
                row = jnp.where(tile < used, row, -1.0)
                row = jnp.broadcast_to(row, (PACK, BLOCK_ROWS)).astype(jnp.bfloat16)
                hit = jnp.where(row[None] == row_ids, one, zero)
                total = hit if total is None else total + hit
            counts.append(total.reshape(BLOCK_ROWS, BLOCK_ROWS))
            blocks.append(turned[tile_block[step * TILES + tile]])
        lhs = jnp.concatenate(blocks, axis=1)
        rhs = jnp.concatenate(counts, axis=0)
        return acc + jnp.dot(lhs, rhs, preferred_element_type=jnp.float32)

    summed = lax.fori_loop(
        0, (used + GROUP - 1) // GROUP, body, jnp.zeros((width, BLOCK_ROWS), jnp.float32)
    )
    mean = summed / (used * FAN_T).astype(jnp.float32)
    out_ref[:, :width] = held[step]
    out_ref[:, width:] = mean.T.astype(jnp.bfloat16)


def aggregate(arrived, slot_of, tile_block, local_nbr, tile_count):
    front = slot_of.shape[0]
    width = arrived.shape[-1]
    dst_blocks = tile_count.shape[0]
    return pl.pallas_call(
        functools.partial(aggregate_kernel, front, width),
        out_shape=jax.ShapeDtypeStruct((dst_blocks * BLOCK_ROWS, 2 * width), jnp.bfloat16),
        grid_spec=pltpu.PrefetchScalarGridSpec(
            num_scalar_prefetch=3,
            grid=(dst_blocks,),
            in_specs=[
                pl.BlockSpec((BLOCK_ROWS, TILES * FAN_T), lambda i, *_: (i, 0)),
                pl.BlockSpec(memory_space=pl.ANY),
            ],
            out_specs=pl.BlockSpec((BLOCK_ROWS, 2 * width), lambda i, *_: (i, 0)),
            scratch_shapes=[
                pltpu.VMEM((front, BLOCK_ROWS, width), jnp.bfloat16),
                pltpu.VMEM((front, width, BLOCK_ROWS), jnp.bfloat16),
                pltpu.VMEM((TILES * FAN_T, BLOCK_ROWS), jnp.float32),
                pltpu.SemaphoreType.DMA((front,)),
            ],
        ),
        compiler_params=pltpu.CompilerParams(dimension_semantics=("arbitrary",)),
        cost_estimate=pl.CostEstimate(flops=4 * 10**9, bytes_accessed=8 * 2**20, transcendentals=0),
    )(slot_of, tile_block.reshape(-1), tile_count, local_nbr, arrived)


def project_kernel(n_col, width, order, x_ref, *rest):
    w_refs = rest[:-1]
    out_ref = rest[-1]
    total = None
    for s in range(n_col):
        rows = x_ref[order[s]]
        term = jnp.dot(rows[:, :width], w_refs[2 * s][...], preferred_element_type=jnp.float32)
        term = term + jnp.dot(rows[:, width:], w_refs[2 * s + 1][...], preferred_element_type=jnp.float32)
        total = term if total is None else total + term
    hidden = jnp.maximum(total, 0.0)
    squares = jnp.sum(hidden * hidden, axis=1, keepdims=True)
    result = (hidden / jnp.sqrt(0.25 + squares / D)).astype(jnp.bfloat16)
    for k in range(n_col):
        out_ref[k] = result[:, k * width : (k + 1) * width]


def project(mixed, weights, order):
    n_col, rows, _ = mixed.shape
    width = D // n_col
    tile = BLOCK_ROWS
    return pl.pallas_call(
        functools.partial(project_kernel, n_col, width),
        out_shape=jax.ShapeDtypeStruct((n_col, rows, width), jnp.bfloat16),
        grid_spec=pltpu.PrefetchScalarGridSpec(
            num_scalar_prefetch=1,
            grid=(rows // tile,),
            in_specs=[pl.BlockSpec((n_col, tile, 2 * width), lambda i, *_: (0, i, 0))]
            + [pl.BlockSpec((width, D), lambda i, *_: (0, 0)) for _ in weights],
            out_specs=pl.BlockSpec((n_col, tile, width), lambda i, *_: (0, i, 0)),
        ),
        compiler_params=pltpu.CompilerParams(dimension_semantics=("arbitrary",)),
        cost_estimate=pl.CostEstimate(flops=2 * 10**9, bytes_accessed=7 * 2**20, transcendentals=0),
    )(order, mixed, *weights)


def on_device(features, requests, counts, tile_block, local_nbr, tile_count, w_self, w_neigh):
    n_dom = lax.axis_size("dom")
    n_col = lax.axis_size("col")
    col_width = features.shape[1]
    blocks = features.reshape(-1, BLOCK_ROWS, col_width)
    weights = [w_self, w_neigh]
    for shift in range(1, n_col):
        perm = [(k, (k + shift) % n_col) for k in range(n_col)]
        weights.append(lax.ppermute(w_self, "col", perm))
        weights.append(lax.ppermute(w_neigh, "col", perm))
    me = lax.axis_index("col")
    order = (me - jnp.arange(n_col, dtype=jnp.int32)) % n_col

    outgoing = blocks.at[requests[0].reshape(-1)].get(mode="promise_in_bounds")
    outgoing = outgoing.reshape(n_dom, CAP, BLOCK_ROWS, col_width)
    arrived = lax.all_to_all(outgoing, "dom", split_axis=0, concat_axis=0, tiled=True)
    arrived = arrived.reshape(n_dom * CAP, BLOCK_ROWS, col_width)
    slot_ends = jnp.cumsum(counts[:, 0])
    positions = jnp.arange(n_dom * CAP // 2, dtype=jnp.int32)
    passed = slot_ends[None, :] <= positions[:, None]
    owner_of = jnp.sum(passed.astype(jnp.int32), axis=1)
    start_of = jnp.max(jnp.where(passed, slot_ends[None, :], 0), axis=1)
    slot_of = owner_of * CAP + positions - start_of

    mixed = aggregate(arrived, slot_of, tile_block, local_nbr, tile_count)
    rows = mixed.shape[0] // n_col
    mixed = mixed.reshape(n_col, rows, 2 * col_width)
    mixed = lax.all_to_all(mixed, "col", split_axis=0, concat_axis=0, tiled=True)
    result = project(mixed, weights, order)
    result = lax.all_to_all(result, "col", split_axis=0, concat_axis=0, tiled=True)
    return result.reshape(-1, col_width)


def solution(mesh):
    return jax.shard_map(
        on_device,
        mesh=mesh,
        in_specs=(
            P("dom", "col"),
            P("dom", None, None),
            P(None, "dom"),
            P("dom", None),
            P("dom", None),
            P("dom"),
            P("col", None),
            P("col", None),
        ),
        out_specs=P("dom", "col"),
        check_vma=False,
    )
```

```python
import functools

import jax
import jax.numpy as jnp
from jax import lax
from jax.experimental import pallas as pl
from jax.experimental.pallas import tpu as pltpu
from jax.sharding import PartitionSpec as P

D = 1024
BLOCK_ROWS = 128
CAP = 8
TILES = 32
FAN_T = 4
GROUP = 4
PACK = 16


def aggregate_kernel(
    front, width, slot_of, tile_block, tile_count, nbr_ref, arrived, out_ref, held, turned, nbr_t, sems
):
    step = pl.program_id(0)

    def fetch(p):
        return pltpu.make_async_copy(arrived.at[slot_of[p]], held.at[p], sems.at[p])

    @pl.when(step == 0)
    def _():
        def begin(p, carry):
            fetch(p).start()
            return carry

        lax.fori_loop(0, front, begin, 0)

        def finish(p, carry):
            fetch(p).wait()
            turned[p] = held[p].T
            return carry

        lax.fori_loop(0, front, finish, 0)

    nbr_t[...] = nbr_ref[...].astype(jnp.float32).T
    used = tile_count[step]
    shape = (BLOCK_ROWS // PACK, PACK, BLOCK_ROWS)
    row_ids = (
        lax.broadcasted_iota(jnp.int32, shape, 0) * PACK + lax.broadcasted_iota(jnp.int32, shape, 1)
    ).astype(jnp.float32).astype(jnp.bfloat16)
    one = jnp.ones(shape, jnp.bfloat16)
    zero = jnp.zeros(shape, jnp.bfloat16)

    def body(q, acc):
        nbr = nbr_t[pl.ds(pl.multiple_of(q * (GROUP * FAN_T), GROUP * FAN_T), GROUP * FAN_T), :]
        counts = []
        blocks = []
        for i in range(GROUP):
            tile = q * GROUP + i
            total = None
            for f in range(FAN_T):
                row = nbr[i * FAN_T + f : i * FAN_T + f + 1, :]
                row = jnp.where(tile < used, row, -1.0)
                row = jnp.broadcast_to(row, (PACK, BLOCK_ROWS)).astype(jnp.bfloat16)
                hit = jnp.where(row[None] == row_ids, one, zero)
                total = hit if total is None else total + hit
            counts.append(total.reshape(BLOCK_ROWS, BLOCK_ROWS))
            blocks.append(turned[tile_block[step * TILES + tile]])
        lhs = jnp.concatenate(blocks, axis=1)
        rhs = jnp.concatenate(counts, axis=0)
        return acc + jnp.dot(lhs, rhs, preferred_element_type=jnp.float32)

    summed = lax.fori_loop(
        0, (used + GROUP - 1) // GROUP, body, jnp.zeros((width, BLOCK_ROWS), jnp.float32)
    )
    mean = summed / (used * FAN_T).astype(jnp.float32)
    out_ref[:, :width] = held[step]
    out_ref[:, width:] = mean.T.astype(jnp.bfloat16)


def aggregate(arrived, slot_of, tile_block, local_nbr, tile_count):
    front = slot_of.shape[0]
    width = arrived.shape[-1]
    dst_blocks = tile_count.shape[0]
    return pl.pallas_call(
        functools.partial(aggregate_kernel, front, width),
        out_shape=jax.ShapeDtypeStruct((dst_blocks * BLOCK_ROWS, 2 * width), jnp.bfloat16),
        grid_spec=pltpu.PrefetchScalarGridSpec(
            num_scalar_prefetch=3,
            grid=(dst_blocks,),
            in_specs=[
                pl.BlockSpec((BLOCK_ROWS, TILES * FAN_T), lambda i, *_: (i, 0)),
                pl.BlockSpec(memory_space=pl.ANY),
            ],
            out_specs=pl.BlockSpec((BLOCK_ROWS, 2 * width), lambda i, *_: (i, 0)),
            scratch_shapes=[
                pltpu.VMEM((front, BLOCK_ROWS, width), jnp.bfloat16),
                pltpu.VMEM((front, width, BLOCK_ROWS), jnp.bfloat16),
                pltpu.VMEM((TILES * FAN_T, BLOCK_ROWS), jnp.float32),
                pltpu.SemaphoreType.DMA((front,)),
            ],
        ),
        compiler_params=pltpu.CompilerParams(dimension_semantics=("arbitrary",)),
        cost_estimate=pl.CostEstimate(flops=4 * 10**9, bytes_accessed=8 * 2**20, transcendentals=0),
    )(slot_of, tile_block.reshape(-1), tile_count, local_nbr, arrived)


def project_kernel(n_col, width, order, x_ref, *rest):
    w_refs = rest[:-1]
    out_ref = rest[-1]
    total = None
    for s in range(n_col):
        rows = x_ref[order[s]]
        term = jnp.dot(rows[:, :width], w_refs[2 * s][...], preferred_element_type=jnp.float32)
        term = term + jnp.dot(rows[:, width:], w_refs[2 * s + 1][...], preferred_element_type=jnp.float32)
        total = term if total is None else total + term
    hidden = jnp.maximum(total, 0.0)
    squares = jnp.sum(hidden * hidden, axis=1, keepdims=True)
    result = (hidden / jnp.sqrt(0.25 + squares / D)).astype(jnp.bfloat16)
    for k in range(n_col):
        out_ref[k] = result[:, k * width : (k + 1) * width]


def project(mixed, weights, order):
    n_col, rows, _ = mixed.shape
    width = D // n_col
    tile = BLOCK_ROWS
    return pl.pallas_call(
        functools.partial(project_kernel, n_col, width),
        out_shape=jax.ShapeDtypeStruct((n_col, rows, width), jnp.bfloat16),
        grid_spec=pltpu.PrefetchScalarGridSpec(
            num_scalar_prefetch=1,
            grid=(rows // tile,),
            in_specs=[pl.BlockSpec((n_col, tile, 2 * width), lambda i, *_: (0, i, 0))]
            + [pl.BlockSpec((width, D), lambda i, *_: (0, 0)) for _ in weights],
            out_specs=pl.BlockSpec((n_col, tile, width), lambda i, *_: (0, i, 0)),
        ),
        compiler_params=pltpu.CompilerParams(dimension_semantics=("arbitrary",)),
        cost_estimate=pl.CostEstimate(flops=2 * 10**9, bytes_accessed=7 * 2**20, transcendentals=0),
    )(order, mixed, *weights)


MESH = pl.DeviceIdType.MESH
CHUNKS = 8
LINE = 4


def exchange_kernel(n_dom, on_line, outgoing, w_self, w_neigh, arrived, far_self, far_neigh, send, recv, own_sem, w_send, w_recv):
    me = lax.axis_index("dom")
    z = lax.axis_index("col")

    def weight_copies(target):
        pairs = ((w_self, far_self), (w_neigh, far_neigh))
        return [
            pltpu.make_async_remote_copy(
                src_ref=src, dst_ref=dst, send_sem=w_send.at[i], recv_sem=w_recv.at[i],
                device_id={"col": target}, device_id_type=MESH,
            )
            for i, (src, dst) in enumerate(pairs)
        ]

    def copy_to(d):
        peer = lax.rem(me + d, n_dom)
        return pltpu.make_async_remote_copy(
            src_ref=outgoing.at[peer], dst_ref=arrived.at[me], send_sem=send.at[d], recv_sem=recv.at[d],
            device_id={"dom": peer}, device_id_type=MESH,
        )

    own = pltpu.make_async_copy(outgoing.at[me], arrived.at[me], own_sem)
    for d in range(1, n_dom):
        copy_to(d).start()
    own.start()
    if on_line:
        toward = 1 + z // 2
        at_end = jnp.logical_or(z == 0, z == LINE - 1)

        @pl.when(at_end)
        def _():
            for copy in weight_copies(toward):
                copy.start()

    own.wait()
    for d in range(1, n_dom):
        copy_to(d).wait_send()
        copy_to(d).wait_recv()
    if on_line:

        @pl.when(at_end)
        def _():
            for copy in weight_copies(toward):
                copy.wait_send()

        @pl.when(jnp.logical_not(at_end))
        def _():
            for copy in weight_copies(toward):
                copy.wait_recv()


def exchange(outgoing, w_self, w_neigh, on_line):
    n_dom = outgoing.shape[0]
    anywhere = pl.BlockSpec(memory_space=pl.ANY)
    return pl.pallas_call(
        functools.partial(exchange_kernel, n_dom, on_line),
        out_shape=[jax.ShapeDtypeStruct(a.shape, a.dtype) for a in (outgoing, w_self, w_neigh)],
        in_specs=[anywhere] * 3,
        out_specs=[anywhere] * 3,
        scratch_shapes=[
            pltpu.SemaphoreType.DMA((n_dom,)),
            pltpu.SemaphoreType.DMA((n_dom,)),
            pltpu.SemaphoreType.DMA,
            pltpu.SemaphoreType.DMA((2,)),
            pltpu.SemaphoreType.DMA((2,)),
        ],
        compiler_params=pltpu.CompilerParams(has_side_effects=True),
    )(outgoing, w_self, w_neigh)


def line_kernel(
    rows, width, mixed, w_self, w_neigh, far_self, far_neigh, out,
    near, part, part_in, kept, sums, sums_in, passed_on,
    near_send, near_recv, part_send, part_recv, sum_send, sum_recv, out_send, out_recv,
):
    z = lax.axis_index("col")
    at_end = jnp.logical_or(z == 0, z == LINE - 1)
    half = z // 2
    span = 2 * width
    mine = pl.ds(pl.multiple_of(half * span, span), span)
    theirs = pl.ds(pl.multiple_of((1 - half) * span, span), span)
    n_chunks = mixed.shape[0] // rows

    def remote(src, dst, s_sem, r_sem, target):
        return pltpu.make_async_remote_copy(
            src_ref=src, dst_ref=dst, send_sem=s_sem, recv_sem=r_sem,
            device_id={"col": target}, device_id_type=MESH,
        )

    def near_copy(c):
        piece = pl.ds(c * rows, rows)
        return remote(mixed.at[piece], near.at[piece], near_send.at[c], near_recv.at[c], 1 + half)

    def part_copy(c):
        return remote(part.at[c], part_in.at[c], part_send.at[c], part_recv.at[c], 2 - half)

    def sum_copy(c):
        return remote(sums.at[c], sums_in.at[c], sum_send.at[c], sum_recv.at[c], 2 - half)

    def out_copy(c):
        piece = pl.ds(c * rows, rows)
        return remote(passed_on.at[c], out.at[piece], out_send.at[c], out_recv.at[c], half * (LINE - 1))

    @pl.when(at_end)
    def _():
        for c in range(n_chunks):
            near_copy(c).start()
        for c in range(n_chunks):
            near_copy(c).wait_send()
        for c in range(n_chunks):
            out_copy(c).wait_recv()

    def product(c, columns):
        piece = pl.ds(c * rows, rows)
        own = mixed[piece, :]
        far = near[piece, :]
        total = jnp.dot(own[:, :width], w_self[:, columns], preferred_element_type=jnp.float32)
        total += jnp.dot(own[:, width:], w_neigh[:, columns], preferred_element_type=jnp.float32)
        total += jnp.dot(far[:, :width], far_self[:, columns], preferred_element_type=jnp.float32)
        total += jnp.dot(far[:, width:], far_neigh[:, columns], preferred_element_type=jnp.float32)
        return total

    def first(c):
        near_copy(c).wait_recv()
        part[c] = product(c, theirs).astype(jnp.bfloat16)
        kept[c] = product(c, mine)
        part_copy(c).start()

    def second(c):
        part_copy(c).wait_recv()
        hidden = jnp.maximum(kept[c] + part_in[c].astype(jnp.float32), 0.0)
        kept[c] = hidden
        squares = jnp.sum(hidden * hidden, axis=1, keepdims=True)
        sums[c] = jnp.broadcast_to(squares, (rows, 128)).T[:8]
        sum_copy(c).start()

    def third(c):
        sum_copy(c).wait_recv()
        squares = (sums[c] + sums_in[c]).T[:, :1]
        result = (kept[c] / jnp.sqrt(0.25 + squares / D)).astype(jnp.bfloat16)
        low, high = result[:, :width], result[:, width:]
        passed_on[c] = jnp.where(half == 0, low, high)
        out[pl.ds(c * rows, rows), :] = jnp.where(half == 0, high, low)
        out_copy(c).start()

    @pl.when(jnp.logical_not(at_end))
    def _():
        for i in range(n_chunks + 2):
            if i < n_chunks:
                first(i)
            if 0 <= i - 1 < n_chunks:
                second(i - 1)
            if 0 <= i - 2:
                third(i - 2)
        for c in range(n_chunks):
            part_copy(c).wait_send()
            sum_copy(c).wait_send()
            out_copy(c).wait_send()


def project_on_line(mixed, w_self, w_neigh, far_self, far_neigh):
    total = mixed.shape[0]
    width = mixed.shape[1] // 2
    rows = total // CHUNKS
    inside = pl.BlockSpec(memory_space=pltpu.VMEM)
    return pl.pallas_call(
        functools.partial(line_kernel, rows, width),
        out_shape=jax.ShapeDtypeStruct((total, width), jnp.bfloat16),
        in_specs=[inside] * 5,
        out_specs=inside,
        scratch_shapes=[
            pltpu.VMEM((total, 2 * width), jnp.bfloat16),
            pltpu.VMEM((CHUNKS, rows, 2 * width), jnp.bfloat16),
            pltpu.VMEM((CHUNKS, rows, 2 * width), jnp.bfloat16),
            pltpu.VMEM((CHUNKS, rows, 2 * width), jnp.float32),
            pltpu.VMEM((CHUNKS, 8, rows), jnp.float32),
            pltpu.VMEM((CHUNKS, 8, rows), jnp.float32),
            pltpu.VMEM((CHUNKS, rows, width), jnp.bfloat16),
        ]
        + [pltpu.SemaphoreType.DMA((CHUNKS,))] * 8,
        compiler_params=pltpu.CompilerParams(has_side_effects=True),
    )(mixed, w_self, w_neigh, far_self, far_neigh)


def on_device(features, requests, counts, tile_block, local_nbr, tile_count, w_self, w_neigh):
    n_dom = lax.axis_size("dom")
    n_col = lax.axis_size("col")
    col_width = features.shape[1]
    blocks = features.reshape(-1, BLOCK_ROWS, col_width)
    on_line = n_col == LINE
    outgoing = blocks.at[requests[0].reshape(-1)].get(mode="promise_in_bounds")
    outgoing = outgoing.reshape(n_dom, CAP, BLOCK_ROWS, col_width)
    arrived, far_self, far_neigh = exchange(outgoing, w_self, w_neigh, on_line)
    arrived = arrived.reshape(n_dom * CAP, BLOCK_ROWS, col_width)
    slot_ends = jnp.cumsum(counts[:, 0])
    positions = jnp.arange(n_dom * CAP // 2, dtype=jnp.int32)
    passed = slot_ends[None, :] <= positions[:, None]
    owner_of = jnp.sum(passed.astype(jnp.int32), axis=1)
    start_of = jnp.max(jnp.where(passed, slot_ends[None, :], 0), axis=1)
    slot_of = owner_of * CAP + positions - start_of

    mixed = aggregate(arrived, slot_of, tile_block, local_nbr, tile_count)
    if on_line:
        return project_on_line(mixed, w_self, w_neigh, far_self, far_neigh)
    weights = [w_self, w_neigh]
    for shift in range(1, n_col):
        perm = [(k, (k + shift) % n_col) for k in range(n_col)]
        weights.append(lax.ppermute(w_self, "col", perm))
        weights.append(lax.ppermute(w_neigh, "col", perm))
    order = (lax.axis_index("col") - jnp.arange(n_col, dtype=jnp.int32)) % n_col
    mixed = mixed.reshape(n_col, -1, 2 * col_width)
    mixed = lax.all_to_all(mixed, "col", split_axis=0, concat_axis=0, tiled=True)
    result = project(mixed, weights, order)
    result = lax.all_to_all(result, "col", split_axis=0, concat_axis=0, tiled=True)
    return result.reshape(-1, col_width)


def solution(mesh):
    return jax.shard_map(
        on_device,
        mesh=mesh,
        in_specs=(
            P("dom", "col"),
            P("dom", None, None),
            P(None, "dom"),
            P("dom", None),
            P("dom", None),
            P("dom"),
            P("col", None),
            P("col", None),
        ),
        out_specs=P("dom", "col"),
        check_vma=False,
    )
```

```python
import functools

import jax
import jax.numpy as jnp
from jax import lax
from jax.experimental import pallas as pl
from jax.experimental.pallas import tpu as pltpu
from jax.sharding import PartitionSpec as P

D = 1024
BLOCK_ROWS = 128
CAP = 8
TILES = 32
FAN_T = 4
GROUP = 8
PACK = 16


def aggregate_kernel(
    front, width, slot_of, tile_block, tile_count, nbr_ref, arrived, out_ref, held, turned, nbr_t, sems
):
    step = pl.program_id(0)

    def fetch(p):
        return pltpu.make_async_copy(arrived.at[slot_of[p]], held.at[p], sems.at[p])

    @pl.when(step == 0)
    def _():
        def begin(p, carry):
            fetch(p).start()
            return carry

        lax.fori_loop(0, front, begin, 0)

        def finish(i, carry):
            for k in range(4):
                fetch(i * 4 + k).wait()
            for k in range(4):
                turned[i * 4 + k] = held[i * 4 + k].T
            return carry

        lax.fori_loop(0, front // 4, finish, 0)

    nbr_t[...] = nbr_ref[...].astype(jnp.float32).T
    used = tile_count[step]
    shape = (BLOCK_ROWS // PACK, PACK, BLOCK_ROWS)
    row_ids = (
        lax.broadcasted_iota(jnp.int32, shape, 0) * PACK + lax.broadcasted_iota(jnp.int32, shape, 1)
    ).astype(jnp.float32).astype(jnp.bfloat16)
    one = jnp.ones(shape, jnp.bfloat16)
    zero = jnp.zeros(shape, jnp.bfloat16)

    def body(q, acc):
        nbr = nbr_t[pl.ds(pl.multiple_of(q * (GROUP * FAN_T), GROUP * FAN_T), GROUP * FAN_T), :]
        counts = []
        blocks = []
        for i in range(GROUP):
            tile = q * GROUP + i
            total = None
            for f in range(FAN_T):
                row = nbr[i * FAN_T + f : i * FAN_T + f + 1, :]
                row = jnp.where(tile < used, row, -1.0)
                row = jnp.broadcast_to(row, (PACK, BLOCK_ROWS)).astype(jnp.bfloat16)
                hit = jnp.where(row[None] == row_ids, one, zero)
                total = hit if total is None else total + hit
            counts.append(total.reshape(BLOCK_ROWS, BLOCK_ROWS))
            blocks.append(turned[tile_block[step * TILES + tile]])
        lhs = jnp.concatenate(blocks, axis=1)
        rhs = jnp.concatenate(counts, axis=0)
        return acc + jnp.dot(lhs, rhs, preferred_element_type=jnp.float32)

    summed = lax.fori_loop(
        0, (used + GROUP - 1) // GROUP, body, jnp.zeros((width, BLOCK_ROWS), jnp.float32)
    )
    mean = summed / (used * FAN_T).astype(jnp.float32)
    out_ref[:, :width] = held[step]
    out_ref[:, width:] = mean.T.astype(jnp.bfloat16)


def aggregate(arrived, slot_of, tile_block, local_nbr, tile_count):
    front = slot_of.shape[0]
    width = arrived.shape[-1]
    dst_blocks = tile_count.shape[0]
    return pl.pallas_call(
        functools.partial(aggregate_kernel, front, width),
        out_shape=jax.ShapeDtypeStruct((dst_blocks * BLOCK_ROWS, 2 * width), jnp.bfloat16),
        grid_spec=pltpu.PrefetchScalarGridSpec(
            num_scalar_prefetch=3,
            grid=(dst_blocks,),
            in_specs=[
                pl.BlockSpec((BLOCK_ROWS, TILES * FAN_T), lambda i, *_: (i, 0)),
                pl.BlockSpec(memory_space=pl.ANY),
            ],
            out_specs=pl.BlockSpec((BLOCK_ROWS, 2 * width), lambda i, *_: (i, 0)),
            scratch_shapes=[
                pltpu.VMEM((front, BLOCK_ROWS, width), jnp.bfloat16),
                pltpu.VMEM((front, width, BLOCK_ROWS), jnp.bfloat16),
                pltpu.VMEM((TILES * FAN_T, BLOCK_ROWS), jnp.float32),
                pltpu.SemaphoreType.DMA((front,)),
            ],
        ),
        compiler_params=pltpu.CompilerParams(dimension_semantics=("arbitrary",)),
        cost_estimate=pl.CostEstimate(flops=4 * 10**9, bytes_accessed=8 * 2**20, transcendentals=0),
    )(slot_of, tile_block.reshape(-1), tile_count, local_nbr, arrived)


def project_kernel(n_col, width, order, x_ref, *rest):
    w_refs = rest[:-1]
    out_ref = rest[-1]
    total = None
    for s in range(n_col):
        rows = x_ref[order[s]]
        term = jnp.dot(rows[:, :width], w_refs[2 * s][...], preferred_element_type=jnp.float32)
        term = term + jnp.dot(rows[:, width:], w_refs[2 * s + 1][...], preferred_element_type=jnp.float32)
        total = term if total is None else total + term
    hidden = jnp.maximum(total, 0.0)
    squares = jnp.sum(hidden * hidden, axis=1, keepdims=True)
    result = (hidden / jnp.sqrt(0.25 + squares / D)).astype(jnp.bfloat16)
    for k in range(n_col):
        out_ref[k] = result[:, k * width : (k + 1) * width]


def project(mixed, weights, order):
    n_col, rows, _ = mixed.shape
    width = D // n_col
    tile = BLOCK_ROWS
    return pl.pallas_call(
        functools.partial(project_kernel, n_col, width),
        out_shape=jax.ShapeDtypeStruct((n_col, rows, width), jnp.bfloat16),
        grid_spec=pltpu.PrefetchScalarGridSpec(
            num_scalar_prefetch=1,
            grid=(rows // tile,),
            in_specs=[pl.BlockSpec((n_col, tile, 2 * width), lambda i, *_: (0, i, 0))]
            + [pl.BlockSpec((width, D), lambda i, *_: (0, 0)) for _ in weights],
            out_specs=pl.BlockSpec((n_col, tile, width), lambda i, *_: (0, i, 0)),
        ),
        compiler_params=pltpu.CompilerParams(dimension_semantics=("arbitrary",)),
        cost_estimate=pl.CostEstimate(flops=2 * 10**9, bytes_accessed=7 * 2**20, transcendentals=0),
    )(order, mixed, *weights)


MESH = pl.DeviceIdType.MESH
CHUNKS = 16
SWAP_LAG = 2
SUM_LAG = 4
LINE = 4


def exchange_kernel(n_dom, on_line, outgoing, w_self, w_neigh, arrived, far_self, far_neigh, send, recv, own_sem, w_send, w_recv):
    me = lax.axis_index("dom")
    z = lax.axis_index("col")

    def weight_copies(target):
        pairs = ((w_self, far_self), (w_neigh, far_neigh))
        return [
            pltpu.make_async_remote_copy(
                src_ref=src, dst_ref=dst, send_sem=w_send.at[i], recv_sem=w_recv.at[i],
                device_id={"col": target}, device_id_type=MESH,
            )
            for i, (src, dst) in enumerate(pairs)
        ]

    def copy_to(d):
        peer = lax.rem(me + d, n_dom)
        return pltpu.make_async_remote_copy(
            src_ref=outgoing.at[peer], dst_ref=arrived.at[me], send_sem=send.at[d], recv_sem=recv.at[d],
            device_id={"dom": peer}, device_id_type=MESH,
        )

    own = pltpu.make_async_copy(outgoing.at[me], arrived.at[me], own_sem)
    for d in range(1, n_dom):
        copy_to(d).start()
    own.start()
    if on_line:
        toward = 1 + z // 2
        at_end = jnp.logical_or(z == 0, z == LINE - 1)

        @pl.when(at_end)
        def _():
            for copy in weight_copies(toward):
                copy.start()

    own.wait()
    for d in range(1, n_dom):
        copy_to(d).wait_send()
        copy_to(d).wait_recv()
    if on_line:

        @pl.when(at_end)
        def _():
            for copy in weight_copies(toward):
                copy.wait_send()

        @pl.when(jnp.logical_not(at_end))
        def _():
            for copy in weight_copies(toward):
                copy.wait_recv()


def exchange(outgoing, w_self, w_neigh, on_line):
    n_dom = outgoing.shape[0]
    anywhere = pl.BlockSpec(memory_space=pl.ANY)
    return pl.pallas_call(
        functools.partial(exchange_kernel, n_dom, on_line),
        out_shape=[jax.ShapeDtypeStruct(a.shape, a.dtype) for a in (outgoing, w_self, w_neigh)],
        in_specs=[anywhere] * 3,
        out_specs=[anywhere] * 3,
        scratch_shapes=[
            pltpu.SemaphoreType.DMA((n_dom,)),
            pltpu.SemaphoreType.DMA((n_dom,)),
            pltpu.SemaphoreType.DMA,
            pltpu.SemaphoreType.DMA((2,)),
            pltpu.SemaphoreType.DMA((2,)),
        ],
        compiler_params=pltpu.CompilerParams(has_side_effects=True),
    )(outgoing, w_self, w_neigh)


def line_kernel(
    rows, width, mixed, w_self, w_neigh, far_self, far_neigh, out,
    near, part, part_in, kept, sums, sums_in, passed_on,
    near_send, near_recv, part_send, part_recv, sum_send, sum_recv, out_send, out_recv,
):
    z = lax.axis_index("col")
    at_end = jnp.logical_or(z == 0, z == LINE - 1)
    half = z // 2
    span = 2 * width
    mine = pl.ds(pl.multiple_of(half * span, span), span)
    theirs = pl.ds(pl.multiple_of((1 - half) * span, span), span)
    n_chunks = mixed.shape[0] // rows

    def remote(src, dst, s_sem, r_sem, target):
        return pltpu.make_async_remote_copy(
            src_ref=src, dst_ref=dst, send_sem=s_sem, recv_sem=r_sem,
            device_id={"col": target}, device_id_type=MESH,
        )

    def near_copy(c):
        piece = pl.ds(c * rows, rows)
        return remote(mixed.at[piece], near.at[piece], near_send.at[c], near_recv.at[c], 1 + half)

    def part_copy(c):
        return remote(part.at[c], part_in.at[c], part_send.at[c], part_recv.at[c], 2 - half)

    def sum_copy(c):
        return remote(sums.at[c], sums_in.at[c], sum_send.at[c], sum_recv.at[c], 2 - half)

    def out_copy(c):
        piece = pl.ds(c * rows, rows)
        return remote(passed_on.at[c], out.at[piece], out_send.at[c], out_recv.at[c], half * (LINE - 1))

    @pl.when(at_end)
    def _():
        for c in range(n_chunks):
            near_copy(c).start()
        for c in range(n_chunks):
            near_copy(c).wait_send()
        for c in range(n_chunks):
            out_copy(c).wait_recv()

    def product(c, columns):
        piece = pl.ds(c * rows, rows)
        own = mixed[piece, :]
        far = near[piece, :]
        total = jnp.dot(own[:, :width], w_self[:, columns], preferred_element_type=jnp.float32)
        total += jnp.dot(own[:, width:], w_neigh[:, columns], preferred_element_type=jnp.float32)
        total += jnp.dot(far[:, :width], far_self[:, columns], preferred_element_type=jnp.float32)
        total += jnp.dot(far[:, width:], far_neigh[:, columns], preferred_element_type=jnp.float32)
        return total

    def first(c):
        near_copy(c).wait_recv()
        part[c] = product(c, theirs).astype(jnp.bfloat16)
        kept[c] = product(c, mine)
        part_copy(c).start()

    def second(c):
        part_copy(c).wait_recv()
        hidden = jnp.maximum(kept[c] + part_in[c].astype(jnp.float32), 0.0)
        kept[c] = hidden
        squares = jnp.sum(hidden * hidden, axis=1, keepdims=True)
        sums[c] = jnp.broadcast_to(squares, (rows, 128)).T[:8]
        sum_copy(c).start()

    def third(c):
        sum_copy(c).wait_recv()
        squares = (sums[c] + sums_in[c]).T[:, :1]
        result = (kept[c] / jnp.sqrt(0.25 + squares / D)).astype(jnp.bfloat16)
        low, high = result[:, :width], result[:, width:]
        passed_on[c] = jnp.where(half == 0, low, high)
        out[pl.ds(c * rows, rows), :] = jnp.where(half == 0, high, low)
        out_copy(c).start()

    @pl.when(jnp.logical_not(at_end))
    def _():
        for i in range(n_chunks + SUM_LAG):
            if i < n_chunks:
                first(i)
            if 0 <= i - SWAP_LAG < n_chunks:
                second(i - SWAP_LAG)
            if 0 <= i - SUM_LAG:
                third(i - SUM_LAG)
        for c in range(n_chunks):
            part_copy(c).wait_send()
            sum_copy(c).wait_send()
            out_copy(c).wait_send()


def project_on_line(mixed, w_self, w_neigh, far_self, far_neigh):
    total = mixed.shape[0]
    width = mixed.shape[1] // 2
    rows = total // CHUNKS
    inside = pl.BlockSpec(memory_space=pltpu.VMEM)
    return pl.pallas_call(
        functools.partial(line_kernel, rows, width),
        out_shape=jax.ShapeDtypeStruct((total, width), jnp.bfloat16),
        in_specs=[inside] * 5,
        out_specs=inside,
        scratch_shapes=[
            pltpu.VMEM((total, 2 * width), jnp.bfloat16),
            pltpu.VMEM((CHUNKS, rows, 2 * width), jnp.bfloat16),
            pltpu.VMEM((CHUNKS, rows, 2 * width), jnp.bfloat16),
            pltpu.VMEM((CHUNKS, rows, 2 * width), jnp.float32),
            pltpu.VMEM((CHUNKS, 8, rows), jnp.float32),
            pltpu.VMEM((CHUNKS, 8, rows), jnp.float32),
            pltpu.VMEM((CHUNKS, rows, width), jnp.bfloat16),
        ]
        + [pltpu.SemaphoreType.DMA((CHUNKS,))] * 8,
        compiler_params=pltpu.CompilerParams(has_side_effects=True),
    )(mixed, w_self, w_neigh, far_self, far_neigh)


def on_device(features, requests, counts, tile_block, local_nbr, tile_count, w_self, w_neigh):
    n_dom = lax.axis_size("dom")
    n_col = lax.axis_size("col")
    col_width = features.shape[1]
    blocks = features.reshape(-1, BLOCK_ROWS, col_width)
    on_line = n_col == LINE
    outgoing = blocks.at[requests[0].reshape(-1)].get(mode="promise_in_bounds")
    outgoing = outgoing.reshape(n_dom, CAP, BLOCK_ROWS, col_width)
    arrived, far_self, far_neigh = exchange(outgoing, w_self, w_neigh, on_line)
    arrived = arrived.reshape(n_dom * CAP, BLOCK_ROWS, col_width)
    slot_ends = jnp.cumsum(counts[:, 0])
    positions = jnp.arange(n_dom * CAP // 2, dtype=jnp.int32)
    passed = slot_ends[None, :] <= positions[:, None]
    owner_of = jnp.sum(passed.astype(jnp.int32), axis=1)
    start_of = jnp.max(jnp.where(passed, slot_ends[None, :], 0), axis=1)
    slot_of = owner_of * CAP + positions - start_of

    mixed = aggregate(arrived, slot_of, tile_block, local_nbr, tile_count)
    if on_line:
        return project_on_line(mixed, w_self, w_neigh, far_self, far_neigh)
    weights = [w_self, w_neigh]
    for shift in range(1, n_col):
        perm = [(k, (k + shift) % n_col) for k in range(n_col)]
        weights.append(lax.ppermute(w_self, "col", perm))
        weights.append(lax.ppermute(w_neigh, "col", perm))
    order = (lax.axis_index("col") - jnp.arange(n_col, dtype=jnp.int32)) % n_col
    mixed = mixed.reshape(n_col, -1, 2 * col_width)
    mixed = lax.all_to_all(mixed, "col", split_axis=0, concat_axis=0, tiled=True)
    result = project(mixed, weights, order)
    result = lax.all_to_all(result, "col", split_axis=0, concat_axis=0, tiled=True)
    return result.reshape(-1, col_width)


def solution(mesh):
    return jax.shard_map(
        on_device,
        mesh=mesh,
        in_specs=(
            P("dom", "col"),
            P("dom", None, None),
            P(None, "dom"),
            P("dom", None),
            P("dom", None),
            P("dom"),
            P("col", None),
            P("col", None),
        ),
        out_specs=P("dom", "col"),
        check_vma=False,
    )
```
